32 devices in a mesh: tp: 8 (over z, y), dp: 4 (over x, core).
Axes of the slice: x: 2, y: 2, z: 4, core: 2. Of those that a mesh axis runs over, the one named last changes fastest.
Arguments:
- x: bfloat16 [8, 1024, 2048], P('dp')
- lengths: int32 [8], P('dp')
- targets: int32 [8], P('dp')
- norm1: bfloat16 [2, 2048], replicated
- norm2: bfloat16 [2, 2048], replicated
- norm_f: bfloat16 [2048], replicated
- w_q: bfloat16 [2, 2048, 16, 128], P(None, ('dp', 'tp'))
- w_k: bfloat16 [2, 2048, 2, 128], P(None, ('dp', 'tp'))
- w_v: bfloat16 [2, 2048, 2, 128], P(None, ('dp', 'tp'))
- w_o: bfloat16 [2, 2048, 2048], P(None, ('dp', 'tp'))
- w_gate: bfloat16 [2, 2048, 11008], P(None, ('dp', 'tp'))
- w_up: bfloat16 [2, 2048, 11008], P(None, ('dp', 'tp'))
- w_down: bfloat16 [2, 11008, 2048], P(None, ('dp', 'tp'))
- w_lm: bfloat16 [2048, 151936], P(('dp', 'tp'))
Outputs:
- output 1: bfloat16 [2, 2048, 16, 128], P(None, None, 'tp')
- output 2: bfloat16 [2, 2048, 8, 128], P(None, None, 'tp')
- output 3: bfloat16 [2, 2048, 8, 128], P(None, None, 'tp')
- output 4: bfloat16 [2, 2048, 2048], P(None, 'tp')
- output 5: bfloat16 [2, 2048, 11008], P(None, None, 'tp')
- output 6: bfloat16 [2, 2048, 11008], P(None, None, 'tp')
- output 7: bfloat16 [2, 11008, 2048], P(None, 'tp')
- output 8: bfloat16 [2, 8, 8, 1024, 128], P(None, 'dp', 'tp')
- output 9: bfloat16 [2, 8, 8, 1024, 128], P(None, 'dp', 'tp')
- output 10: float32 [8], P('dp')
All inputs are finite; a program needn't handle non-finite values.
Results may differ from the reference program's by a relative error of at most 0.0117063.
Values are sent between devices in bfloat16 or wider.
A program may use at most 1 GiB of HBM per device.

```python
import jax
import jax.numpy as jnp
from jax import lax

MODEL_DIM = 2048
Q_HEADS = 16
KV_HEADS = 2
HEAD_DIM = 128
FFN_DIM = 11008
VOCAB_SIZE = 151936
SEQ_LEN = 1024
NUM_LAYERS = 2
TP_SIZE = 8
BATCH_ALL = 8

ROPE_BASE = 10000.0
NORM_EPS = 1e-6


def draw_normal(rng_key, shape, scale):
    return (jax.random.normal(rng_key, shape, jnp.float32) * scale).astype(jnp.bfloat16)


def draw_gain(rng_key, shape):
    return jax.random.uniform(rng_key, shape, jnp.float32, 0.5, 1.5).astype(jnp.bfloat16)


def setup_inputs(seed: int = 0) -> dict:
    subkeys = jax.random.split(jax.random.key(seed), 16)
    q_width = Q_HEADS * HEAD_DIM
    lengths = jax.random.randint(subkeys[0], (BATCH_ALL,), SEQ_LEN // 4, SEQ_LEN + 1, jnp.int32)
    full_at = jax.random.randint(subkeys[1], (), 0, BATCH_ALL, jnp.int32)
    lengths = jnp.where(jnp.arange(BATCH_ALL) == full_at, SEQ_LEN, lengths).astype(jnp.int32)
    targets = jax.random.randint(subkeys[2], (BATCH_ALL,), 0, VOCAB_SIZE, jnp.int32)
    dim_scale = MODEL_DIM ** -0.5
    return dict(
        x=draw_normal(subkeys[3], (BATCH_ALL, SEQ_LEN, MODEL_DIM), 1.0),
        lengths=lengths,
        targets=targets,
        norm1=draw_gain(subkeys[4], (NUM_LAYERS, MODEL_DIM)),
        norm2=draw_gain(subkeys[5], (NUM_LAYERS, MODEL_DIM)),
        norm_f=draw_gain(subkeys[6], (MODEL_DIM,)),
        w_q=draw_normal(subkeys[7], (NUM_LAYERS, MODEL_DIM, Q_HEADS, HEAD_DIM), 2.0 * dim_scale),
        w_k=draw_normal(subkeys[8], (NUM_LAYERS, MODEL_DIM, KV_HEADS, HEAD_DIM), dim_scale),
        w_v=draw_normal(subkeys[9], (NUM_LAYERS, MODEL_DIM, KV_HEADS, HEAD_DIM), dim_scale),
        w_o=draw_normal(subkeys[10], (NUM_LAYERS, q_width, MODEL_DIM), 2.0 * q_width ** -0.5),
        w_gate=draw_normal(subkeys[11], (NUM_LAYERS, MODEL_DIM, FFN_DIM), dim_scale),
        w_up=draw_normal(subkeys[12], (NUM_LAYERS, MODEL_DIM, FFN_DIM), dim_scale),
        w_down=draw_normal(subkeys[13], (NUM_LAYERS, FFN_DIM, MODEL_DIM), FFN_DIM ** -0.5),
        w_lm=draw_normal(subkeys[14], (MODEL_DIM, VOCAB_SIZE), 2.0 * dim_scale),
    )


def rms_scale(hidden, gain):
    hidden32 = hidden.astype(jnp.float32)
    inv_rms = lax.rsqrt(jnp.mean(hidden32 * hidden32, axis=-1, keepdims=True) + NORM_EPS)
    return (hidden32 * inv_rms * gain.astype(jnp.float32)).astype(jnp.bfloat16)


def rope_tables():
    positions = jnp.arange(SEQ_LEN, dtype=jnp.float32)
    inv_freq = ROPE_BASE ** (-2.0 * jnp.arange(HEAD_DIM // 2, dtype=jnp.float32) / HEAD_DIM)
    angles = positions[:, None] * inv_freq[None, :]
    return jnp.cos(angles), jnp.sin(angles)


def apply_rope(projected, cos_tab, sin_tab):
    half_dim = projected.shape[-1] // 2
    lower_half = projected[..., :half_dim]
    upper_half = projected[..., half_dim:]
    cos_rows = cos_tab[:, None, :]
    sin_rows = sin_tab[:, None, :]
    return jnp.concatenate([lower_half * cos_rows - upper_half * sin_rows, upper_half * cos_rows + lower_half * sin_rows], axis=-1)


def residual_add(hidden, update):
    return (hidden.astype(jnp.float32) + update.astype(jnp.float32)).astype(jnp.bfloat16)


def reference(x, lengths, targets, norm1, norm2, norm_f, w_q, w_k, w_v, w_o, w_gate, w_up, w_down, w_lm):
    cos_tab, sin_tab = rope_tables()
    positions = jnp.arange(SEQ_LEN)
    group_size = Q_HEADS // KV_HEADS
    replicas = TP_SIZE // KV_HEADS
    score_scale = HEAD_DIM ** -0.5
    layer_weights = (norm1, norm2, w_q, w_k, w_v, w_o, w_gate, w_up, w_down)

    def one_sequence(seq_args):
        hidden, length, target = seq_args
        visible = (positions[None, :] <= positions[:, None]) & (positions[None, :] < length)

        def layer_step(resid, weights):
            gain_attn, gain_mlp, wq_l, wk_l, wv_l, wo_l, wg_l, wu_l, wd_l = weights
            normed = rms_scale(resid, gain_attn)
            q_proj = jnp.dot(normed, wq_l.reshape(MODEL_DIM, Q_HEADS * HEAD_DIM), preferred_element_type=jnp.float32)
            q_rot = apply_rope(q_proj.reshape(SEQ_LEN, Q_HEADS, HEAD_DIM), cos_tab, sin_tab).astype(jnp.bfloat16)
            k_proj = jnp.dot(normed, wk_l.reshape(MODEL_DIM, KV_HEADS * HEAD_DIM), preferred_element_type=jnp.float32)
            k_rot = apply_rope(k_proj.reshape(SEQ_LEN, KV_HEADS, HEAD_DIM), cos_tab, sin_tab).astype(jnp.bfloat16)
            v_proj = jnp.dot(normed, wv_l.reshape(MODEL_DIM, KV_HEADS * HEAD_DIM), preferred_element_type=jnp.float32)
            v_proj = v_proj.astype(jnp.bfloat16).reshape(SEQ_LEN, KV_HEADS, HEAD_DIM)
            q_grp = q_rot.reshape(SEQ_LEN, KV_HEADS, group_size, HEAD_DIM).astype(jnp.float32)
            scores = jnp.einsum('skgd,tkd->kgst', q_grp, k_rot.astype(jnp.float32)) * score_scale
            scores = jnp.where(visible, scores, -1e30)
            attn_probs = jax.nn.softmax(scores, axis=-1).astype(jnp.bfloat16)
            attn_mix = jnp.einsum('kgst,tkd->skgd', attn_probs.astype(jnp.float32), v_proj.astype(jnp.float32)).astype(jnp.bfloat16)
            attn_out = jnp.dot(attn_mix.reshape(SEQ_LEN, Q_HEADS * HEAD_DIM), wo_l, preferred_element_type=jnp.float32).astype(jnp.bfloat16)
            resid = residual_add(resid, attn_out)
            normed2 = rms_scale(resid, gain_mlp)
            gate_proj = jnp.dot(normed2, wg_l, preferred_element_type=jnp.float32)
            up_proj = jnp.dot(normed2, wu_l, preferred_element_type=jnp.float32)
            activated = (jax.nn.silu(gate_proj) * up_proj).astype(jnp.bfloat16)
            down_out = jnp.dot(activated, wd_l, preferred_element_type=jnp.float32).astype(jnp.bfloat16)
            resid = residual_add(resid, down_out)
            return resid, (jnp.swapaxes(k_rot, 0, 1), jnp.swapaxes(v_proj, 0, 1))

        final, (k_layers, v_layers) = lax.scan(layer_step, hidden, layer_weights)
        last_row = lax.dynamic_slice_in_dim(final, length - 1, 1, axis=0)
        logits = jnp.dot(rms_scale(last_row, norm_f), w_lm, preferred_element_type=jnp.float32)[0]
        logprob = lax.dynamic_index_in_dim(logits, target, keepdims=False) - jax.nn.logsumexp(logits)
        return k_layers, v_layers, logprob

    k_all, v_all, logprob = lax.map(one_sequence, (x, lengths, targets))
    k_cache = jnp.repeat(jnp.swapaxes(k_all, 0, 1), replicas, axis=2)
    v_cache = jnp.repeat(jnp.swapaxes(v_all, 0, 1), replicas, axis=2)
    k_out = jnp.repeat(w_k, replicas, axis=2)
    v_out = jnp.repeat(w_v, replicas, axis=2)
    return (w_q, k_out, v_out, w_o, w_gate, w_up, w_down, k_cache, v_cache, logprob)
```

```python
import jax
import jax.numpy as jnp
from jax import lax
from jax.experimental import pallas as pl
from jax.experimental.pallas import tpu as pltpu
from jax.sharding import PartitionSpec as P

ROPE_BASE = 10000.0
NORM_EPS = 1e-6
F32 = jnp.float32
BF16 = jnp.bfloat16
MESH_ID = pl.DeviceIdType.MESH
ANYWHERE = pl.BlockSpec(memory_space=pl.ANY)
IN_VMEM = pl.BlockSpec(memory_space=pltpu.VMEM)

MIB = 1 << 20


def place_of():
    tp, dp = lax.axis_index('tp'), lax.axis_index('dp')
    return tp, dp, tp // 2, tp % 2


def traffic(count):
    return pl.CostEstimate(flops=0, bytes_accessed=count, transcendentals=0)


def everyone(tp, dp):
    return [((tp + i) % 8, (dp + j) % 4) for j in range(4) for i in range(8) if i or j]


def shifted(z, y, dz, dy):
    return ((z + dz) % 4) * 2 + (y + dy) % 2


def send_to(src, dst, ss, rs, t, d):
    return pltpu.make_async_remote_copy(src_ref=src, dst_ref=dst, send_sem=ss, recv_sem=rs, device_id={'tp': t, 'dp': d}, device_id_type=MESH_ID)


def greet(others):
    barrier = pltpu.get_barrier_semaphore()
    for t, d in others:
        pl.semaphore_signal(barrier, inc=1, device_id={'tp': t, 'dp': d}, device_id_type=MESH_ID)
    pl.semaphore_wait(barrier, len(others))


def spread(groups, hop=False):
    chunks = [(g, r) for g, group in enumerate(groups) for r in range(len(group))]
    count = len(chunks)
    high = [group[0].shape[0] for group in groups]

    def steps(ins, outs, scratch):
        (sh, rh, sx, rx, sp, rp, sf, rf, keep) = scratch
        tp, dp, z, y = place_of()
        xn = (dp + 2) % 4
        cn = dp + 1 - 2 * (dp % 2)

        def spot(n, d):
            g, r = chunks[n]
            place = d if len(groups[g]) == 1 else d * 8 + shifted(z, y, 4 - r // 2, 2 - r % 2)
            return outs[g].at[pl.ds(place * high[g], high[g])]

        started = []

        def go(src, dst, s, r, d):
            c = send_to(src, dst, s, r, tp, d)
            c.start()
            started.append(c)

        kept = []

        def keep_copy(n):
            return pltpu.make_async_copy(ins[n], spot(n, dp), keep.at[n])

        def hand_on(n, src):
            go(src, spot(n, dp), sx.at[n], rx.at[n], xn)
            go(src, spot(n, dp), sp.at[n], rp.at[n], cn)

        def owned(n):
            return hop and chunks[n][1] > 0

        def row_hop(n):
            t, d = dp * 2 + tp // 4, tp % 4
            g = chunks[n][0]
            dst = outs[g].at[pl.ds(d * high[g], high[g])]
            return send_to(ins[n], dst, sh.at[n], rh.at[n], t, d)

        at_home = jnp.logical_and(dp * 2 + tp // 4 == tp, tp % 4 == dp)
        away = jnp.logical_not(at_home)

        rows = [n for n in range(count) if hop and len(groups[chunks[n][0]]) == 1]
        for n in range(count):
            g, r = chunks[n]
            if owned(n):
                dst = outs[g].at[pl.ds((dp * 8 + tp) * high[g], high[g])]
                c = send_to(ins[n], dst, sh.at[n], rh.at[n], shifted(z, y, r // 2, r % 2), dp)
                c.start()
                started.append(c)
            elif n in rows:
                pl.when(at_home)(keep_copy(n).start)
                pl.when(away)(row_hop(n).start)
        for n in range(count):
            if not owned(n) and n not in rows:
                hand_on(n, ins[n])
                kept.append(keep_copy(n))
                kept[-1].start()
        for n in range(count):
            here = spot(n, dp)
            if owned(n):
                yield
                send_to(here, here, sh.at[n], rh.at[n], tp, cn).wait_recv()
                hand_on(n, here)
            elif n in rows:
                yield
                pl.when(at_home)(keep_copy(n).wait)
                pl.when(away)(send_to(here, here, sh.at[n], rh.at[n], tp, cn).wait_recv)
                hand_on(n, here)
        for n in range(count):
            there = spot(n, xn)
            yield
            send_to(there, there, sx.at[n], rx.at[n], tp, xn).wait_recv()
            go(there, there, sf.at[n], rf.at[n], cn)
        yield
        for n in range(count):
            near, far = spot(n, cn), spot(n, (cn + 2) % 4)
            send_to(near, near, sp.at[n], rp.at[n], tp, cn).wait_recv()
            send_to(far, far, sf.at[n], rf.at[n], tp, cn).wait_recv()
        for c in started:
            c.wait_send()
        for c in kept:
            c.wait()
        for n in rows:
            pl.when(away)(row_hop(n).wait_send)

    dma = pltpu.SemaphoreType.DMA((count,))
    outs = [jax.ShapeDtypeStruct((4 * len(group) * group[0].shape[0], group[0].shape[1]), BF16) for group in groups]
    moved = sum(c.size for group in groups for c in group) * 80
    return dict(ins=[c for group in groups for c in group], in_space=IN_VMEM, outs=outs, out_space=ANYWHERE, scratch=[dma] * 9, steps=steps, far=True, wide=hop, turns=count + 2, moved=moved)


WAYS = (1, -1)
HOPS = (1, 2, 3)


def on_line(z):
    return jnp.logical_and(z >= 0, z < 4)


def lane_of_copies(s, r, tp, dp):
    slots, sent = {}, []

    def slot(key):
        return slots.setdefault(key, len(slots))

    def go(src, dst, key, t, when=None):
        c = send_to(src, dst, s.at[slot(key)], r.at[slot(key)], t, dp)
        sent.append((c, when))
        c.start() if when is None else pl.when(when)(c.start)

    def got(dst, key, when=None):
        c = send_to(dst, dst, s.at[slot(key)], r.at[slot(key)], tp, dp)
        c.wait_recv() if when is None else pl.when(when)(c.wait_recv)

    def finish():
        for c, when in sent:
            c.wait_send() if when is None else pl.when(when)(c.wait_send)

    return go, got, finish


def gather_tokens(block):
    rows, width = block.shape
    second = rows // 4
    first = rows - second

    def steps(ins, outs, scratch):
        own, out, (s, r, keep) = ins[0], outs[0], scratch
        tp, dp, z, y = place_of()
        yn = 1 - y
        t_y = z * 2 + yn
        go, got, finish = lane_of_copies(s, r, tp, dp)
        spans = {'a': (0, first), 'b': (first, second)}

        def at(zz, yy, part):
            off, n = spans[part]
            return out.at[pl.ds(((zz + 4) % 4 * 2 + yy) * rows + off, n)]

        def mine(part):
            return own.at[pl.ds(*spans[part])]

        def pass_on(way, k, part, yy, src=None):
            there = at(z - way * k, yy, part)
            to = (z + way + 4) % 4 * 2 + y
            go(there if src is None else src, there, (part, yy is y, way, k), to, jnp.logical_and(on_line(z - way * k), on_line(z + way)))

        go(mine('b'), at(z, y, 'b'), 'y', t_y)
        for part in spans:
            for way in WAYS:
                pass_on(way, 0, part, y, mine(part))
        go(mine('a'), at(z, y, 'a'), 'ya', t_y)
        stay = pltpu.make_async_copy(own, out.at[pl.ds(tp * rows, rows)], keep)
        stay.start()
        yield
        got(at(z, yn, 'b'), 'y')
        for way in WAYS:
            pass_on(way, 0, 'b', yn)
        for k in HOPS:
            for part, yy in (('a', y), ('b', y), ('b', yn)):
                for way in WAYS:
                    here = on_line(z - way * k)
                    there = at(z - way * k, yy, part)
                    yield
                    got(there, (part, yy is y, way, k - 1), here)
                    if k < HOPS[-1]:
                        pass_on(way, k, part, yy)
                    if part == 'a':
                        go(there, there, ('ya', way, k), t_y, here)
        yield
        got(at(z, yn, 'a'), 'ya')
        for k in HOPS:
            for way in WAYS:
                got(at(z - way * k, yn, 'a'), ('ya', way, k), on_line(z - way * k))
        finish()
        stay.wait()

    dma = pltpu.SemaphoreType.DMA
    outs = [jax.ShapeDtypeStruct((8 * rows, width), block.dtype)]
    return dict(ins=[block], in_space=ANYWHERE, outs=outs, out_space=ANYWHERE, scratch=[dma((32,)), dma((32,)), dma], steps=steps, far=False, wide=False, turns=20, moved=block.size * 150)


def scatter_sum(part):
    total, width = part.shape
    rows = total // 8
    second = rows // 4
    first = rows - second

    def steps(ins, outs, scratch):
        p, out, (yb, ua, ma, ub, mb, tb, cb, s, r) = ins[0], outs[0], scratch
        tp, dp, z, y = place_of()
        yn = 1 - y
        t_y = z * 2 + yn
        go, got, finish = lane_of_copies(s, r, tp, dp)

        def early(zz, yy):
            return p.at[pl.ds(((zz + 4) % 4 * 2 + yy) * rows, first)]

        def late(zz, yy):
            return p.at[pl.ds(((zz + 4) % 4 * 2 + yy) * rows + first, second)]

        def add(*refs):
            acc = refs[0][...].astype(F32)
            for ref in refs[1:]:
                acc = acc + ref[...].astype(F32)
            return acc.astype(BF16)

        far_first = HOPS[::-1]
        for k in far_first:
            for way in WAYS:
                t = z + way * k
                go(early(t, yn), yb.at[(t + 4) % 4], ('y', way, k), t_y, on_line(t))
        go(early(z, yn), yb.at[z], 'y', t_y)

        for side, way in enumerate(WAYS):
            for k in range(3):
                def clear():
                    ua[side, k] = jnp.zeros((first, width), BF16)
                    ub[side, k] = jnp.zeros((2, second, width), BF16)
                comes = jnp.logical_and(on_line(z - way), on_line(z + way * k))
                pl.when(jnp.logical_not(comes))(clear)

        def expected(way, k):
            return jnp.logical_and(on_line(z - way), on_line(z + way * k))

        for k in far_first:
            for side, way in enumerate(WAYS):
                t = z + way * k
                to = (z + way + 4) % 4 * 2 + y
                yield
                if k < HOPS[-1]:
                    for yy in range(2):
                        got(ub.at[side, k, yy], ('b', way, k, yy), expected(way, k))

                def sum_late():
                    for yy in range(2):
                        extra = [ub.at[side, k, yy]] if k < HOPS[-1] else []
                        mb[side, k - 1, yy] = add(late(t, yy), *extra)
                pl.when(on_line(t))(sum_late)
                for yy in range(2):
                    go(mb.at[side, k - 1, yy], ub.at[side, k - 1, yy], ('b', way, k - 1, yy), to, on_line(t))
            for side, way in enumerate(WAYS):
                t = z + way * k
                to = (z + way + 4) % 4 * 2 + y
                yield
                got(yb.at[(t + 4) % 4], ('y', way, k), on_line(t))
                if k < HOPS[-1]:
                    got(ua.at[side, k], ('a', way, k), expected(way, k))

                def sum_early():
                    extra = [ua.at[side, k]] if k < HOPS[-1] else []
                    ma[side, k - 1] = add(early(t, y), yb.at[(t + 4) % 4], *extra)
                pl.when(on_line(t))(sum_early)
                go(ma.at[side, k - 1], ua.at[side, k - 1], ('a', way, k - 1), to, on_line(t))
        yield
        for yy in range(2):
            for side, way in enumerate(WAYS):
                got(ub.at[side, 0, yy], ('b', way, 0, yy), on_line(z - way))
            tb[yy] = add(late(z, yy), *[ub.at[side, 0, yy] for side in range(2)])
        go(tb.at[yn], cb, 'late', t_y)
        yield
        got(yb.at[z], 'y')
        for side, way in enumerate(WAYS):
            got(ua.at[side, 0], ('a', way, 0), on_line(z - way))
        out[:first] = add(early(z, y), yb.at[z], *[ua.at[side, 0] for side in range(2)])
        yield
        got(cb, 'late')
        out[first:] = add(tb.at[y], cb)
        finish()

    dma = pltpu.SemaphoreType.DMA
    V = lambda *shape: pltpu.VMEM(shape + (width,), BF16)
    outs = [jax.ShapeDtypeStruct((rows, width), BF16)]
    scratch = [V(4, first), V(2, 3, first), V(2, 3, first), V(2, 3, 2, second), V(2, 3, 2, second), V(2, second), V(second), dma((32,)), dma((32,))]
    return dict(ins=[part], in_space=IN_VMEM, outs=outs, out_space=IN_VMEM, scratch=scratch, steps=steps, far=False, wide=False, turns=16, moved=part.size * 20)


def run_parts(parts, collective_id):
    counts = [(len(c['ins']), len(c['outs']), len(c['scratch'])) for c in parts]

    def kernel(*refs):
        refs = list(refs)

        def take(n):
            taken = refs[:n]
            del refs[:n]
            return taken

        ins = [take(n) for n, _, _ in counts]
        outs = [take(n) for _, n, _ in counts]
        scratch = [take(n) for _, _, n in counts]
        tp, dp, z, y = place_of()
        near = any(not c['far'] for c in parts)
        peers = [(shifted(z, y, dz, dy), dp) for dz, dy in ((1, 0), (3, 0), (0, 1))] if near else []
        if any(c['far'] for c in parts):
            peers += [(tp, (dp + 2) % 4), (tp, dp + 1 - 2 * (dp % 2))]
        greet(everyone(tp, dp) if any(c['wide'] for c in parts) else peers)
        live = [[0, c['turns'], c['steps'](*refs_of)] for c, *refs_of in zip(parts, ins, outs, scratch)]
        while live:
            live.sort(key=lambda entry: entry[0] / entry[1])
            entry = live[0]
            entry[0] += 1
            if next(entry[2], 'end') == 'end':
                live.remove(entry)

    results = pl.pallas_call(
        kernel,
        out_shape=[o for c in parts for o in c['outs']],
        in_specs=[c['in_space'] for c in parts for _ in c['ins']],
        out_specs=[c['out_space'] for c in parts for _ in c['outs']],
        scratch_shapes=[s for c in parts for s in c['scratch']],
        compiler_params=pltpu.CompilerParams(collective_id=collective_id, has_side_effects=True, vmem_limit_bytes=48 * MIB),
        cost_estimate=traffic(sum(c['moved'] for c in parts)),
        name=f'moves{collective_id}',
    )(*[a for c in parts for a in c['ins']])
    grouped = []
    for c in parts:
        grouped.append(results[:len(c['outs'])])
        results = results[len(c['outs']):]
    return grouped


def small_sum(part, collective_id):
    def kernel(own, out, buf, s, r):
        tp, dp, z, y = place_of()
        peers = [(tp + k) % 8 for k in range(1, 8)]
        greet([(t, dp) for t in peers])
        copies = []
        for k, t in enumerate(peers):
            c = send_to(own, buf.at[tp], s.at[k], r.at[k], t, dp)
            c.start()
            copies.append(c)
        buf[tp] = own[...]
        for c in copies:
            c.wait_recv()
        out[...] = sum(buf[t] for t in range(len(peers) + 1))
        for c in copies:
            c.wait_send()

    vmem = pl.BlockSpec(memory_space=pltpu.VMEM)
    n = 7
    return pl.pallas_call(
        kernel,
        out_shape=jax.ShapeDtypeStruct(part.shape, part.dtype),
        in_specs=[vmem],
        out_specs=vmem,
        scratch_shapes=[pltpu.VMEM((n + 1,) + part.shape, part.dtype), pltpu.SemaphoreType.DMA((n,)), pltpu.SemaphoreType.DMA((n,))],
        compiler_params=pltpu.CompilerParams(collective_id=collective_id, has_side_effects=True),
        name=f'smallsum{collective_id}',
    )(part)


def vocab_logprob(part, targets, vocab, collective_id):
    batch, padded = part.shape
    colors = (0, 1)
    sizes = [padded // 2 >> k for k in range(1, 4)]
    chunk = sizes[-1] // 4

    def kernel(p, tgt, out, *scratch):
        got, total_of = scratch[:3], scratch[3:6]
        rz, own_stats, stats, s, r, ss, rs = scratch[6:]
        tp, dp, z, y = place_of()
        x, c = dp // 2, dp % 2
        greet(everyone(tp, dp))
        copies = []
        core, along_x, along_y = (c, tp, dp + 1 - 2 * c), (x, tp, (dp + 2) % 4), (y, z * 2 + 1 - y, dp)
        dims = ((core, along_x, along_y), (core, along_y, along_x))

        def go(src, dst, s_sem, r_sem, t, d):
            cp = send_to(src, dst, s_sem, r_sem, t, d)
            cp.start()
            copies.append(cp)
            return cp

        def lanes(ref, index, n):
            return ref.at[:, pl.ds(pl.multiple_of(index * n, 128), n)]

        now = [lanes(p, k, padded // 2) for k in colors]
        base = [k * (padded // 2) for k in colors]
        for stage, n in enumerate(sizes):
            flying = []
            for k in colors:
                bit, t, d = dims[k][stage]
                flying.append(go(lanes(now[k], 1 - bit, n), got[stage].at[k], s.at[k, stage], r.at[k, stage], t, d))
            for k in colors:
                bit = dims[k][stage][0]
                flying[k].wait_recv()
                total_of[stage][k] = (lanes(now[k], bit, n)[...].astype(F32) + got[stage][k].astype(F32)).astype(BF16)
                now[k] = total_of[stage].at[k]
                base[k] = base[k] + bit * n
        last = []
        for k in colors:
            for turn in range(1, 4):
                there = (z + turn) % 4
                last.append((k, turn, go(lanes(now[k], there, chunk), rz.at[k, turn], s.at[k, 2 + turn], r.at[k, 2 + turn], there * 2 + y, dp)))
        logits = [lanes(now[k], z, chunk)[...].astype(F32) for k in colors]
        for k, turn, cp in last:
            cp.wait_recv()
            logits[k] = logits[k] + rz[k, turn].astype(F32)
        lane = lax.broadcasted_iota(jnp.int32, (batch, chunk), 1)
        ids = jnp.concatenate([base[k] + z * chunk + lane for k in colors], axis=1)
        logits = jnp.where(ids < vocab, jnp.concatenate(logits, axis=1), -jnp.inf)
        top = jnp.max(logits, axis=1, keepdims=True)
        safe = jnp.where(top == -jnp.inf, 0.0, top)
        total = jnp.sum(jnp.exp(logits - safe), axis=1, keepdims=True)
        hit = jnp.sum(jnp.where(ids == tgt[...], logits, 0.0), axis=1, keepdims=True)
        spot = lane[:, :128]
        own_stats[...] = jnp.where(spot == 0, top, jnp.where(spot == 1, total, hit))
        sends = []
        for k, (t, d) in enumerate(everyone(tp, dp)):
            sends.append(go(own_stats, stats.at[dp * 8 + tp], ss.at[k], rs.at[k], t, d))
        stats[dp * 8 + tp] = own_stats[...]
        for cp in sends:
            cp.wait_recv()
        every = stats[...]
        tops, sums, hits = (every[:, :, k:k + 1] for k in range(3))
        peak = jnp.max(tops, axis=0)
        norm_sum = jnp.sum(sums * jnp.exp(tops - peak[None]), axis=0)
        out[...] = jnp.broadcast_to(jnp.sum(hits, axis=0) - peak - jnp.log(norm_sum), (batch, 128))
        for cp in copies:
            cp.wait_send()

    V = lambda *shape: pltpu.VMEM(shape, BF16)
    dma = pltpu.SemaphoreType.DMA
    stage_buffers = [V(2, batch, n) for n in sizes]
    return pl.pallas_call(
        kernel,
        out_shape=jax.ShapeDtypeStruct((batch, 128), F32),
        in_specs=[IN_VMEM, IN_VMEM],
        out_specs=IN_VMEM,
        scratch_shapes=stage_buffers + stage_buffers + [V(2, 4, batch, chunk), pltpu.VMEM((batch, 128), F32), pltpu.VMEM((32, batch, 128), F32), dma((2, 6)), dma((2, 6)), dma((32,)), dma((32,))],
        compiler_params=pltpu.CompilerParams(collective_id=collective_id, has_side_effects=True, vmem_limit_bytes=40 * MIB),
        name=f'vocab{collective_id}',
    )(part, targets)


def column_pieces(parts, layer, after=()):
    tp_size = 8
    rows = parts[0].shape[1]
    totals = [p.shape[2] for p in parts]
    widths = [t // tp_size for t in totals]
    wides = [-(-w // 128) * 128 for w in widths]
    step = 16

    def kernel(*refs):
        out = refs[-1]
        z, y = place_of()[2:]
        for t in range(tp_size):
            turn = shifted(t // 2, t % 2, 4 - z, 2 - y)
            at = 0
            for ref, width, wide in zip(refs, widths, wides):
                out[turn, :, at:at + width] = ref[0, :, t * width:(t + 1) * width]
                if wide > width:
                    out[turn, :, at + width:at + wide] = jnp.zeros((step, wide - width), BF16)
                at += wide

    return pl.pallas_call(
        kernel,
        grid=(rows // step,),
        out_shape=jax.ShapeDtypeStruct((tp_size, rows, sum(wides)), BF16),
        in_specs=[pl.BlockSpec((1, step, t), lambda r: (layer, r, 0)) for t in totals] + [ANYWHERE] * len(after),
        out_specs=pl.BlockSpec((tp_size, step, sum(wides)), lambda r: (0, r, 0)),
        cost_estimate=traffic(sum(totals) * rows * 4),
        name=f'pieces{layer}',
    )(*parts, *after)


def assemble(cols, downs, width):
    layers = len(cols)
    rows = cols[0].shape[0]
    wide = -(-width // 128) * 128
    model_dim = downs[0].shape[1]
    grid, fold = 16, 4
    step, tall = rows // grid, width // fold

    def kernel(*refs):
        gate, up, down = refs[2 * layers:]
        for layer in range(layers):
            gate[layer] = refs[layer][:, :wide].T[:width]
            up[layer] = refs[layer][:, wide:2 * wide].T[:width]

        @pl.when(pl.program_id(0) % fold == 0)
        def _():
            for layer in range(layers):
                down[layer] = refs[layers + layer][...]

    return pl.pallas_call(
        kernel,
        grid=(grid,),
        out_shape=[jax.ShapeDtypeStruct((layers, width, rows), BF16)] * 2 + [jax.ShapeDtypeStruct((layers, width, model_dim), BF16)],
        in_specs=[pl.BlockSpec((step, 2 * wide), lambda i: (i, 0))] * layers + [pl.BlockSpec((tall, model_dim), lambda i: (i // fold, 0))] * layers,
        out_specs=[pl.BlockSpec((layers, width, step), lambda i: (0, 0, i))] * 2 + [pl.BlockSpec((layers, tall, model_dim), lambda i: (0, i // fold, 0))],
        cost_estimate=traffic(12 * layers * rows * width),
        name='assemble',
    )(*cols, *downs)


def feed_forward(tokens, gate_up, down):
    count, model_dim = tokens.shape
    width = down.shape[0]
    wide = -(-width // 128) * 128
    step = 256

    def kernel(rows, gu, dn, out):
        both = jnp.dot(rows[...], gu[...], preferred_element_type=F32)
        gate, up = both[:, :wide], both[:, wide:]
        act = (gate * jax.nn.sigmoid(gate) * up).astype(BF16)[:, :width]
        out[...] = jnp.dot(act, dn[...], preferred_element_type=F32).astype(BF16)

    whole = lambda shape: pl.BlockSpec(shape, lambda i: (0, 0), pipeline_mode=pl.Buffered(1))
    return pl.pallas_call(
        kernel,
        grid=(count // step,),
        out_shape=jax.ShapeDtypeStruct((count, model_dim), BF16),
        in_specs=[pl.BlockSpec((step, model_dim), lambda i: (i, 0)), whole((model_dim, 2 * wide)), whole(down.shape)],
        out_specs=pl.BlockSpec((step, model_dim), lambda i: (i, 0)),
        compiler_params=pltpu.CompilerParams(vmem_limit_bytes=56 * MIB),
        cost_estimate=pl.CostEstimate(flops=6 * count * model_dim * width, bytes_accessed=count * model_dim * 4 + gate_up.size * 2 + down.size * 2, transcendentals=count * width),
        name='feed_forward',
    )(tokens, gate_up, down)


def rms_scale(hidden, gain):
    hidden32 = hidden.astype(F32)
    inv_rms = lax.rsqrt(jnp.mean(hidden32 * hidden32, axis=-1, keepdims=True) + NORM_EPS)
    return (hidden32 * inv_rms * gain.astype(F32)).astype(BF16)


def rope_angles(positions, head_dim):
    inv_freq = ROPE_BASE ** (-2.0 * jnp.arange(head_dim // 2, dtype=F32) / head_dim)
    angles = positions.astype(F32)[:, None] * inv_freq[None, :]
    return jnp.cos(angles), jnp.sin(angles)


def apply_rope(projected, cos_rows, sin_rows):
    half_dim = projected.shape[-1] // 2
    lower_half = projected[..., :half_dim]
    upper_half = projected[..., half_dim:]
    return jnp.concatenate([lower_half * cos_rows - upper_half * sin_rows, upper_half * cos_rows + lower_half * sin_rows], axis=-1)


def residual_add(hidden, update):
    return (hidden.astype(F32) + update.astype(F32)).astype(BF16)


def behind(value, token):
    first = token.reshape(-1)[:1].reshape((1,) * value.ndim)
    return jnp.where(first == first, value, jnp.zeros_like(value))


def dot32(a, b):
    return jnp.dot(a, b, preferred_element_type=F32)


def solution(mesh):
    tp_size = mesh.shape['tp']
    dp_size = mesh.shape['dp']
    row_moves = [(t * dp_size + d, (d * 2 + t // dp_size) * dp_size + t % dp_size) for t in range(tp_size) for d in range(dp_size)]

    def device_program(x, lengths, targets, norm1, norm2, norm_f, w_q, w_k, w_v, w_o, w_gate, w_up, w_down, w_lm):
        tp_idx = lax.axis_index('tp')
        dp_idx = lax.axis_index('dp')
        layers, q_heads, head_dim = w_q.shape[0], w_q.shape[2], w_q.shape[3]
        kv_heads = w_k.shape[2]
        kv_width = kv_heads * head_dim
        replicas = tp_size // kv_heads
        batch, seq_len, model_dim = x.shape
        local_heads = q_heads // tp_size
        score_scale = head_dim ** -0.5
        tokens = batch * seq_len
        shard = tokens // tp_size
        rows_in = w_k.shape[1]
        my_head = tp_idx // replicas

        q_flat = w_q.reshape(layers, rows_in, q_heads * head_dim)
        k_flat = w_k.reshape(layers, rows_in, kv_width)
        v_flat = w_v.reshape(layers, rows_in, kv_width)

        turns = [(dz, dy) for dz in range(4) for dy in range(2)]

        def along(piece_of):
            received = [piece_of(0)]
            for r, (dz, dy) in enumerate(turns):
                if r:
                    perm = [(t, shifted(t // 2, t % 2, dz, dy)) for t in range(tp_size)]
                    received.append(lax.ppermute(piece_of(r), 'tp', perm))
            return received

        def to_owner(local_rows):
            return [lax.ppermute(local_rows, ('tp', 'dp'), row_moves)]

        def early_piece(r):
            dz, dy = turns[r]
            t = shifted(tp_idx // 2, tp_idx % 2, dz, dy)
            cut = lambda a, start, n: lax.dynamic_slice_in_dim(a, start, n, axis=1)
            head = t // replicas
            return jnp.concatenate([cut(q_flat[0], t * local_heads * head_dim, local_heads * head_dim), cut(k_flat[0], head * head_dim, head_dim), cut(v_flat[0], head * head_dim, head_dim)], axis=1)

        ((qkv0, wo0),) = run_parts([spread([[early_piece(r) for r in range(tp_size)], [w_o[0]]], hop=True)], 1)
        pieces0 = column_pieces([w_gate, w_up], 0, (wo0,))
        gu_chunks, d_chunk = along(lambda r: pieces0[r]), to_owner(behind(w_down[0], wo0))
        local_width = local_heads * head_dim
        wq0, wk0, wv0 = qkv0[:, :local_width], qkv0[:, local_width:local_width + head_dim], qkv0[:, local_width + head_dim:]

        positions = jnp.arange(seq_len)
        cos_tab, sin_tab = rope_angles(positions, head_dim)
        x_rows = x.reshape(tokens, model_dim)

        normed = rms_scale(x_rows, norm1[0])
        q_rot = apply_rope(dot32(normed, wq0).reshape(batch, seq_len, local_heads, head_dim), cos_tab[:, None, :], sin_tab[:, None, :]).astype(BF16)
        k_rot = apply_rope(dot32(normed, wk0).reshape(batch, seq_len, head_dim), cos_tab, sin_tab).astype(BF16)
        v_proj = dot32(normed, wv0).astype(BF16).reshape(batch, seq_len, head_dim)
        causal = positions[None, :] <= positions[:, None]
        visible = (causal[None] & (positions[None, None, :] < lengths[:, None, None]))[:, None]
        scores = jnp.einsum('bshe,bte->bhst', q_rot, k_rot, preferred_element_type=F32) * score_scale
        scores = jnp.where(visible, scores, -1e30)
        attn_probs = jax.nn.softmax(scores, axis=-1).astype(BF16)
        attn_mix = jnp.einsum('bhst,bte->bshe', attn_probs, v_proj, preferred_element_type=F32).astype(BF16)
        attn_part = dot32(attn_mix.reshape(tokens, local_heads * head_dim), wo0).astype(BF16)
        (attn_sum,), (gu0, wd0) = run_parts([scatter_sum(attn_part), spread([gu_chunks, d_chunk])], 2)
        pieces1 = column_pieces([w_gate, w_up, q_flat], 1, (attn_part,))
        cols_chunks = along(lambda r: pieces1[r])
        kv_full = lax.all_gather(behind(jnp.concatenate([k_flat[1], v_flat[1]], axis=1), attn_part), ('dp', 'tp'), axis=0, tiled=True)
        my_rows = lax.dynamic_slice_in_dim(x_rows, tp_idx * shard, shard, axis=0)
        hidden = residual_add(my_rows, attn_sum)

        ((normed,),) = run_parts([gather_tokens(rms_scale(hidden, norm2[0]))], 3)
        rows_chunk = to_owner(behind(jnp.concatenate([w_o[1], w_down[1]], axis=0), normed))
        down_part = feed_forward(normed, gu0, wd0)
        (down_sum,), (cols1, rows1) = run_parts([scatter_sum(down_part), spread([cols_chunks, rows_chunk])], 4)
        width = wd0.shape[0]
        wide = -(-width // 128) * 128
        rows1 = rows1.reshape(dp_size, -1, model_dim)
        o_rows = w_o.shape[1]
        wo1, wd1 = rows1[:, :o_rows].reshape(-1, model_dim), rows1[:, o_rows:].reshape(-1, model_dim)
        hidden = residual_add(hidden, down_sum)

        normed = rms_scale(hidden, norm1[1])
        shards_per_seq = seq_len // shard
        shard_start = (tp_idx % shards_per_seq) * shard
        cos_mine = lax.dynamic_slice_in_dim(cos_tab, shard_start, shard, axis=0)
        sin_mine = lax.dynamic_slice_in_dim(sin_tab, shard_start, shard, axis=0)
        kv_proj = dot32(normed, kv_full)
        k_mine = apply_rope(kv_proj[:, :kv_width].reshape(shard, kv_heads, head_dim), cos_mine[:, None, :], sin_mine[:, None, :]).astype(BF16)
        kv_mine = jnp.concatenate([k_mine.reshape(shard, kv_width), kv_proj[:, kv_width:].astype(BF16)], axis=1)
        kv_all = lax.all_gather(kv_mine, 'tp', axis=0, tiled=True)
        k_rot1 = lax.dynamic_slice_in_dim(kv_all, my_head * head_dim, head_dim, axis=1).reshape(batch, seq_len, head_dim)
        v_proj1 = lax.dynamic_slice_in_dim(kv_all, kv_width + my_head * head_dim, head_dim, axis=1).reshape(batch, seq_len, head_dim)

        last_pos = lengths - 1
        my_tokens = tp_idx * shard + jnp.arange(shard)
        pick = (my_tokens[None, :] == (jnp.arange(batch) * seq_len + last_pos)[:, None]).astype(BF16)
        row = small_sum(dot32(pick, hidden), 5).astype(BF16)
        normed = rms_scale(row, norm1[1])
        cos_last, sin_last = rope_angles(last_pos, head_dim)
        q_last = apply_rope(dot32(normed, cols1[:, 2 * wide:]).reshape(batch, local_heads, head_dim), cos_last[:, None, :], sin_last[:, None, :]).astype(BF16)
        scores = jnp.einsum('bhe,bte->bht', q_last, k_rot1, preferred_element_type=F32) * score_scale
        scores = jnp.where((positions[None, :] <= last_pos[:, None])[:, None, :], scores, -1e30)
        probs = jax.nn.softmax(scores, axis=-1).astype(BF16)
        mix = jnp.einsum('bht,bte->bhe', probs, v_proj1, preferred_element_type=F32).astype(BF16)
        attn_row = small_sum(dot32(mix.reshape(batch, local_heads * head_dim), wo1), 6).astype(BF16)
        row = residual_add(row, attn_row)
        normed = rms_scale(row, norm2[1])
        both = dot32(normed, cols1)
        activated = (jax.nn.silu(both[:, :wide]) * both[:, wide:2 * wide]).astype(BF16)[:, :width]
        down_row = small_sum(dot32(activated, wd1), 7).astype(BF16)
        row = residual_add(row, down_row)

        ride = jnp.broadcast_to(targets.astype(F32)[:, None], (batch, 128))
        carried = lax.all_gather(jnp.concatenate([rms_scale(row, norm_f).astype(F32), ride], axis=1), 'dp', axis=0, tiled=True)
        feats = carried[:, :model_dim].astype(BF16)
        all_targets = carried[:, model_dim:model_dim + 1].astype(jnp.int32)
        lm_rows = w_lm.shape[0]
        dev_idx = dp_idx * tp_size + tp_idx
        feats_mine = lax.dynamic_slice_in_dim(feats, dev_idx * lm_rows, lm_rows, axis=1)
        vocab = w_lm.shape[1]
        chunk = -(-vocab // (128 * tp_size * dp_size)) * 128
        logits_part = jnp.pad(dot32(feats_mine, w_lm).astype(BF16), ((0, 0), (0, chunk * tp_size * dp_size - vocab)))
        logprob_all = vocab_logprob(logits_part, all_targets, vocab, 8)[:, 0]
        logprob = lax.dynamic_slice_in_dim(logprob_all, dp_idx * batch, batch, axis=0)

        k_caches = jnp.stack([k_rot, k_rot1])[:, :, None]
        v_caches = jnp.stack([v_proj, v_proj1])[:, :, None]
        q_out = jnp.stack([wq0, cols1[:, 2 * wide:]]).reshape(layers, model_dim, local_heads, head_dim)
        gate_out, up_out, down_out = assemble([gu0, cols1], [wd0, wd1], width)
        mine = lambda a: lax.dynamic_slice_in_dim(a, my_head * head_dim, head_dim, axis=1)
        k_out = jnp.stack([wk0, mine(kv_full[:, :kv_width])])[:, :, None, :]
        v_out = jnp.stack([wv0, mine(kv_full[:, kv_width:])])[:, :, None, :]
        return (q_out, k_out, v_out, jnp.stack([wo0, wo1]), jnp.swapaxes(gate_out, 1, 2), jnp.swapaxes(up_out, 1, 2), down_out, k_caches, v_caches, logprob)

    row_split = P(None, ('dp', 'tp'), None)
    head_rows = P(None, ('dp', 'tp'), None, None)
    head_cols = P(None, None, 'tp', None)
    col_split = P(None, None, 'tp')
    row_tp = P(None, 'tp', None)
    cache_spec = P(None, 'dp', 'tp', None, None)
    in_specs = (P('dp', None, None), P('dp'), P('dp'), P(), P(), P(), head_rows, head_rows, head_rows, row_split, row_split, row_split, row_split, P(('dp', 'tp'), None))
    out_specs = (head_cols, head_cols, head_cols, row_tp, col_split, col_split, row_tp, cache_spec, cache_spec, P('dp'))
    return jax.shard_map(device_program, mesh=mesh, in_specs=in_specs, out_specs=out_specs, check_vma=False)
```
